32 devices in a mesh: px: 4 (over z), py: 8 (over y, x, core).
Axes of the slice: x: 2, y: 2, z: 4, core: 2. Of those that a mesh axis runs over, the one named last changes fastest.
Arguments:
- features: bfloat16 [24576, 768], P(('px', 'py')), may hold values from -6 to 6
- weight_one: bfloat16 [768, 768], replicated, may hold values from -0.21875 to 0.21875
- weight_two: bfloat16 [768, 768], replicated, may hold values from -0.21875 to 0.21875
- tile_values: bfloat16 [1024, 128, 128], P(('px', 'py')), may hold values from -0.375 to 0.375
- tile_rows: int32 [32, 32], P(('px', 'py')), may hold values from 0 to 5
- tile_cols: int32 [32, 32], P(('px', 'py')), may hold values from 0 to 7
- tile_count: int32 [32], P(('px', 'py')), may hold values from 4 to 32, as said below
- send_rows: int32 [32, 32, 8], P(('px', 'py')), may hold values from 0 to 767
- send_count: int32 [32, 32], P(('px', 'py')), may hold values from 1 to 8, as said below
- stale_hidden: bfloat16 [8192, 768], P(('px', 'py')), may hold values from -3 to 3
- stale_grad: bfloat16 [8192, 768], P(('px', 'py')), may hold values from -6 to 6
- out_grad: bfloat16 [24576, 768], P(('px', 'py')), may hold values from -6 to 6
Outputs:
- next_hidden: bfloat16 [8192, 768], P(('px', 'py'))
- next_grad: bfloat16 [8192, 768], P(('px', 'py'))
- grad_one: float32 [768, 768], replicated
- grad_two: float32 [768, 768], replicated
The draws below stay inside these ranges and needn't reach their ends.
Inputs may be any that keep to these rules, and one draw needn't show every extreme that they name: The tiles of a part with index below its tile_count are live, the others are ignored; some part has 32 live tiles in every draw. `tile_cols`: column tiles below 6 hold the part's own rows; the rest hold the received boundary rows, 8 slots from each part in order of the part. `send_rows`: slots at or beyond the matching send_count are unused. `send_count`: every part sends 8 rows to at least one peer in every draw.
All inputs are finite; a program needn't handle non-finite values.
Results may differ from the reference program's by a relative error of at most 0.0061.
Values may be sent and summed in bfloat16 or wider, within the bound.
A program may use at most 128 MiB of HBM per device.

```python
import math
import jax
import jax.numpy as jnp
from jax import lax

D = 768
ROWS = 768
TILE = 128
TILES = 32
SLOTS = 8
PARTS_SIZE = 32
NODES = 24576
COLTILES = 8
N_PX = 4
N_PY = 8


def draw_tile_count(key, part):
    parts = N_PX * N_PY
    counts = jax.random.randint(jax.random.fold_in(key, 11), (parts,), max(1, TILES // 8), TILES // 2 + 1)
    busiest = jax.random.randint(jax.random.fold_in(key, 12), (), 0, parts)
    return jnp.where(jnp.arange(parts, dtype=jnp.int32) == busiest, TILES, counts).astype(jnp.int32)


def draw_send_count(key, part):
    parts = N_PX * N_PY
    counts = jax.random.randint(jax.random.fold_in(key, 21), (parts, parts), 1, SLOTS + 1)
    fullest = jax.random.randint(jax.random.fold_in(key, 22), (parts,), 0, parts)
    peers = jnp.arange(parts, dtype=jnp.int32)
    return jnp.where(peers[None, :] == fullest[:, None], SLOTS, counts).astype(jnp.int32)


def plant(array, key, low, largest):
    place = [jax.random.randint(jax.random.fold_in(key, axis), (), 0, length) for axis, length in enumerate(array.shape)]
    main_axis = array.shape.index(max(array.shape))
    next_to = place[:main_axis] + [(place[main_axis] + 1) % array.shape[main_axis]] + place[main_axis + 1:]
    return array.at[tuple(place)].set(low).at[tuple(next_to)].set(largest)


def block_levels(stream_key, shape, shards, low, top_value):
    def one(axis_at, shards_of):
        steps = jax.random.uniform(jax.random.fold_in(jax.random.fold_in(stream_key, 6), axis_at), (shards_of,), jnp.float32, low / len(shards), top_value / len(shards))
        return jnp.repeat(jnp.exp(steps), shape[axis_at] // shards_of).reshape((-1,) + (1,) * (len(shape) - axis_at - 1))

    level = one(*shards[0])
    for cut in shards[1:]:
        level = level * one(*cut)
    return level


def normal_values(key, extent, spread, most, split=(), held_as=jnp.bfloat16):
    result = jax.random.normal(key, extent, jnp.float32) * spread
    if len(split) > 0:
        result = block_levels(key, extent, split, -0.22, 0.18) * result
    return jnp.clip(result, min=-most, max=most).astype(held_as)


def setup_inputs(seed: int = 0) -> dict:
    splits = jax.random.split(jax.random.key(seed), 13)
    features = normal_values(splits[0], (NODES, D), 1.0, 6.0, ((0, 32),))
    weight_one = normal_values(splits[1], (D, D), D ** -0.5, 0.21875)
    weight_two = normal_values(splits[2], (D, D), D ** -0.5, 0.21875)
    tile_values = normal_values(splits[3], (PARTS_SIZE * TILES, TILE, TILE), (TILE * 2) ** -0.5, 0.375, ((0, 32),))
    tile_rows = plant(jax.random.randint(splits[4], (PARTS_SIZE, TILES), 0, ROWS // TILE), jax.random.fold_in(splits[4], 1), 0, (ROWS // TILE) - 1).astype(jnp.int32)
    tile_cols = plant(jax.random.randint(splits[5], (PARTS_SIZE, TILES), 0, COLTILES), jax.random.fold_in(splits[5], 1), 0, COLTILES - 1).astype(jnp.int32)
    tile_count = draw_tile_count(jax.random.fold_in(splits[12], 71), 0)
    send_rows = plant(jax.random.randint(splits[7], (PARTS_SIZE, PARTS_SIZE, SLOTS), 0, ROWS), jax.random.fold_in(splits[7], 1), 0, ROWS - 1).astype(jnp.int32)
    send_count = draw_send_count(jax.random.fold_in(splits[12], 71), 0)
    stale_hidden = normal_values(splits[9], (PARTS_SIZE * PARTS_SIZE * SLOTS, D), 0.5, 3.0, ((0, 32),))
    stale_grad = normal_values(splits[10], (PARTS_SIZE * PARTS_SIZE * SLOTS, D), 1.0, 6.0, ((0, 32),))
    out_grad = normal_values(splits[11], (NODES, D), 1.0, 6.0, ((0, 32),))
    return {"features": features, "weight_one": weight_one, "weight_two": weight_two, "tile_values": tile_values, "tile_rows": tile_rows, "tile_cols": tile_cols, "tile_count": tile_count, "send_rows": send_rows, "send_count": send_count, "stale_hidden": stale_hidden, "stale_grad": stale_grad, "out_grad": out_grad}


def exact_gelu(value):
    return jax.nn.gelu(value, approximate=False)

def aggregate(source, tiles, rows, cols, live):
    active = jnp.arange(tiles.shape[0], dtype=jnp.int32) < live
    values = jnp.where(active[:, None, None], tiles, jnp.zeros_like(tiles)).astype(jnp.float32)
    blocks = source.reshape(-1, TILE, D)[cols].astype(jnp.float32)
    partial_value = jnp.einsum('gij,gjd->gid', values, blocks, precision=lax.Precision.HIGHEST)
    return jax.ops.segment_sum(partial_value, rows, num_segments=ROWS // TILE).reshape(ROWS, D)

def spread_back(grads, tiles, rows, cols, live, col_tiles):
    active = jnp.arange(tiles.shape[0], dtype=jnp.int32) < live
    values = jnp.where(active[:, None, None], tiles, jnp.zeros_like(tiles)).astype(jnp.float32)
    blocks = grads.reshape(-1, TILE, D)[rows].astype(jnp.float32)
    partial_value = jnp.einsum('gji,gjd->gid', values, blocks, precision=lax.Precision.HIGHEST)
    return jax.ops.segment_sum(partial_value, cols, num_segments=col_tiles).reshape(-1, D)

def reference(features, weight_one, weight_two, tile_values, tile_rows, tile_cols, tile_count, send_rows, send_count, stale_hidden, stale_grad, out_grad):
    parts = N_PX * N_PY
    col_tiles = (ROWS + parts * SLOTS) // TILE
    slot_ids = jnp.arange(SLOTS, dtype=jnp.int32)
    sent_mask = slot_ids[None, None, :] < send_count[:, :, None]
    heard_mask = jnp.swapaxes(sent_mask, 0, 1)
    own = features.reshape(parts, ROWS, D)

    def pick(item):
        block, chosen = item
        return block[chosen]
    outgoing = lax.map(pick, (own, send_rows))
    outgoing = jnp.where(sent_mask[..., None], outgoing, jnp.zeros_like(outgoing))
    incoming = jnp.swapaxes(outgoing, 0, 1)

    def local_pass(carry, item):
        feats, tiles, rows, cols, live, chosen, sent, arrived, heard, old_hidden, old_grad, cotangent = item
        source_one = jnp.concatenate([feats, arrived.reshape(-1, D)], axis=0)
        agg_one = aggregate(source_one, tiles, rows, cols, live).astype(jnp.bfloat16)
        pre_one = jnp.dot(agg_one, weight_one, preferred_element_type=jnp.float32)
        hidden = exact_gelu(pre_one).astype(jnp.bfloat16)
        picked = hidden[chosen]
        box_hidden = jnp.where(sent[:, :, None], picked, jnp.zeros_like(picked))
        kept = jnp.where(heard.reshape(-1, 1), old_hidden, jnp.zeros_like(old_hidden))
        source_two = jnp.concatenate([hidden, kept], axis=0)
        agg_two = aggregate(source_two, tiles, rows, cols, live).astype(jnp.bfloat16)
        down = jnp.dot(cotangent, weight_two.T, preferred_element_type=jnp.float32).astype(jnp.bfloat16)
        back = spread_back(down, tiles, rows, cols, live, col_tiles)
        own_grad = back[:ROWS]
        remote = back[ROWS:].reshape(parts, SLOTS, D)
        box_grad = jnp.where(heard[:, :, None], remote, jnp.zeros_like(remote)).astype(jnp.bfloat16)
        old_back = old_grad.astype(jnp.float32)
        old_back = jnp.where(sent.reshape(-1, 1), old_back, jnp.zeros_like(old_back))
        hidden_grad = own_grad + jax.ops.segment_sum(old_back, chosen.reshape(-1), num_segments=ROWS)
        pull = jax.vjp(exact_gelu, pre_one)[1]
        pre_grad = pull(hidden_grad)[0].astype(jnp.bfloat16)
        part_one = jnp.dot(agg_one.T, pre_grad, preferred_element_type=jnp.float32)
        part_two = jnp.dot(agg_two.T, cotangent, preferred_element_type=jnp.float32)
        return ((carry[0] + part_one, carry[1] + part_two), (box_hidden, box_grad))
    items = (own, tile_values.reshape(parts, TILES, TILE, TILE), tile_rows, tile_cols, tile_count, send_rows, sent_mask, incoming, heard_mask, stale_hidden.reshape(parts, parts * SLOTS, D), stale_grad.reshape(parts, parts * SLOTS, D), out_grad.reshape(parts, ROWS, D))
    start = (jnp.zeros((D, D), jnp.float32), jnp.zeros((D, D), jnp.float32))
    sums, boxes = lax.scan(local_pass, start, items)
    scale = 1.0 / math.sqrt(ROWS * parts)
    next_hidden = jnp.swapaxes(boxes[0], 0, 1).reshape(-1, D)
    next_grad = jnp.swapaxes(boxes[1], 0, 1).reshape(-1, D)
    return (next_hidden, next_grad, sums[0] * scale, sums[1] * scale)
```

```python
import functools
import math

import jax
import jax.numpy as jnp
from jax import lax
from jax.experimental import pallas as pl
from jax.experimental.pallas import tpu as pltpu
from jax.sharding import PartitionSpec as P

MESH = pl.DeviceIdType.MESH
BF16 = jnp.bfloat16
F32 = jnp.float32


def split_axis(size):
    out, stride = [], 1
    while size > 1:
        two = size & (size - 1) == 0
        step = size if not two else (2 if (size.bit_length() - 1) % 2 else 4)
        out.append((stride, step))
        stride *= step
        size //= step
    return out


def positions(npx, npy):
    px, py = lax.axis_index("px"), lax.axis_index("py")
    return px, py, px * npy + py


def entry_barrier(me, npx, npy):
    parts = npx * npy
    barrier = pltpu.get_barrier_semaphore()

    def greet(step, carry):
        peer = lax.rem(me + step, parts)
        pl.semaphore_signal(
            barrier, inc=1, device_id=(peer // npy, lax.rem(peer, npy)), device_id_type=MESH
        )
        return carry

    lax.fori_loop(1, parts, greet, 0)
    pl.semaphore_wait(barrier, parts - 1)


def start_exchange(me, npx, npy, pairs, send_sem, recv_sem):
    parts = npx * npy

    def send(step, carry):
        peer = lax.rem(me + step, parts)
        for k, (src, dst) in enumerate(pairs):
            pltpu.make_async_remote_copy(
                src_ref=src.at[peer],
                dst_ref=dst.at[me],
                send_sem=send_sem.at[k],
                recv_sem=recv_sem.at[k],
                device_id=(peer // npy, lax.rem(peer, npy)),
                device_id_type=MESH,
            ).start()
        return carry

    lax.fori_loop(1, parts, send, 0)
    for src, dst in pairs:
        dst[me] = src[me]


def finish_exchange(parts, pairs, send_sem, recv_sem):
    for k, (src, dst) in enumerate(pairs):
        part_of = dst.at[pl.ds(0, parts - 1)]
        pltpu.make_async_copy(part_of, part_of, recv_sem.at[k]).wait()
        part_of = src.at[pl.ds(0, parts - 1)]
        pltpu.make_async_copy(part_of, part_of, send_sem.at[k]).wait()


def exchange_kernel(npx, npy, count, *refs):
    srcs, dsts = refs[:count], refs[count : 2 * count]
    send_sem, recv_sem = refs[2 * count :]
    px, py, me = positions(npx, npy)
    entry_barrier(me, npx, npy)
    pairs = list(zip(srcs, dsts))
    start_exchange(me, npx, npy, pairs, send_sem, recv_sem)
    finish_exchange(npx * npy, pairs, send_sem, recv_sem)


def exchange(npx, npy, arrays, collective_id):
    vmem = pl.BlockSpec(memory_space=pltpu.VMEM)
    n = len(arrays)
    return pl.pallas_call(
        functools.partial(exchange_kernel, npx, npy, n),
        out_shape=tuple(jax.ShapeDtypeStruct(a.shape, a.dtype) for a in arrays),
        in_specs=[vmem] * n,
        out_specs=(vmem,) * n,
        scratch_shapes=[pltpu.SemaphoreType.DMA((n,)), pltpu.SemaphoreType.DMA((n,))],
        compiler_params=pltpu.CompilerParams(
            collective_id=collective_id, has_side_effects=True, vmem_limit_bytes=40 * 2**20
        ),
        name="exchange",
    )(*arrays)


def reduce_orders(npx, npy):
    dims = [("py", s, k) for s, k in split_axis(npy)] + [("px", s, k) for s, k in split_axis(npx)]
    near = [d for d in dims if d[2] == 2]
    far = [d for d in dims if d[2] != 2]
    return [near + far, near + far[::-1]]


class Stream:
    def __init__(self, order, parts, px, py, src, out, curs, recvs, sems):
        self.order, self.src, self.out, self.curs, self.recvs = order, src, out, curs, recvs
        self.send_sem, self.recv_sem, self.at = sems
        self.px, self.py = px, py
        self.coord, self.span, left = [], [], parts
        for axis, stride, size in order:
            index = px if axis == "px" else py
            self.coord.append(lax.rem(index // stride, size))
            left //= size
            self.span.append(left)
        self.base, total = [], 0
        for c, n in zip(self.coord, self.span):
            total = total + c * n
            self.base.append(total)
        self.live = {}

    def peer(self, stage, offset):
        axis, stride, size = self.order[stage]
        mine = self.coord[stage]
        other = lax.rem(mine + offset, size)
        move = (other - mine) * stride
        where = (self.px + move, self.py) if axis == "px" else (self.px, self.py + move)
        return other, where

    def copies(self, key, stage, make):
        made = []
        for offset in range(1, self.order[stage][2]):
            other, where = self.peer(stage, offset)
            src, dst = make(offset, other)
            copy = pltpu.make_async_remote_copy(
                src_ref=src,
                dst_ref=dst,
                send_sem=self.send_sem.at[self.at],
                recv_sem=self.recv_sem.at[self.at],
                device_id=where,
                device_id_type=MESH,
            )
            self.at += 1
            copy.start()
            made.append(copy)
        self.live[key] = made

    def scatter_start(self, stage):
        n = self.span[stage]
        cur = self.src if stage == 0 else self.curs[stage - 1]
        self.copies(
            ("rs", stage),
            stage,
            lambda offset, other: (cur.at[pl.ds(other * n, n)], self.recvs[stage].at[offset - 1]),
        )

    def scatter_finish(self, stage):
        n = self.span[stage]
        cur = self.src if stage == 0 else self.curs[stage - 1]
        last = stage == len(self.order) - 1
        target = self.out if last else self.curs[stage]
        start = self.base[stage] if last else 0
        for copy in self.live[("rs", stage)]:
            copy.wait_recv()
        mine = self.coord[stage] * n
        size = self.order[stage][2]

        def add(i, carry):
            total = cur[mine + i].astype(F32)
            for offset in range(1, size):
                total = total + self.recvs[stage][offset - 1, i].astype(F32)
            target[start + i] = total.astype(BF16)
            return carry

        lax.fori_loop(0, n, add, 0)

    def gather_start(self, stage):
        n = self.span[stage]
        block = self.out.at[pl.ds(self.base[stage], n)]
        self.copies(("ag", stage), stage, lambda offset, other: (block, block))

    def gather_finish(self, stage):
        for copy in self.live[("ag", stage)]:
            copy.wait_recv()

    def drain(self):
        for made in self.live.values():
            for copy in made:
                copy.wait_send()


def scratch_for(order, parts, height, width):
    curs, recvs, left = [], [], parts
    for stage, (_, _, size) in enumerate(order):
        left //= size
        recvs.append(pltpu.VMEM((size - 1, left, height, width), BF16))
        if stage < len(order) - 1:
            curs.append(pltpu.VMEM((left, height, width), BF16))
    return curs, recvs


def sum_kernel(npx, npy, box, part_one, part_two, got, out_one, out_two, *scratch):
    parts = npx * npy
    px, py, me = positions(npx, npy)
    orders = reduce_orders(npx, npy)
    stages = len(orders[0])
    box_send, box_recv, red_send, red_recv = scratch[-4:]
    per = 2 * sum(size - 1 for _, _, size in orders[0])
    streams, at = [], 0
    for k, (order, src, out) in enumerate(zip(orders, (part_one, part_two), (out_one, out_two))):
        curs = scratch[at : at + stages - 1]
        recvs = scratch[at + stages - 1 : at + 2 * stages - 1]
        at += 2 * stages - 1
        streams.append(
            Stream(order, parts, px, py, src, out, curs, recvs, (red_send, red_recv, k * per))
        )
    entry_barrier(me, npx, npy)
    for s in streams:
        s.scatter_start(0)
    start_exchange(me, npx, npy, [(box, got)], box_send, box_recv)
    for stage in range(stages):
        for s in streams:
            s.scatter_finish(stage)
            if stage < stages - 1:
                s.scatter_start(stage + 1)
            else:
                s.gather_start(stage)
    for stage in range(stages - 1, -1, -1):
        for s in streams:
            s.gather_finish(stage)
            if stage > 0:
                s.gather_start(stage - 1)
    finish_exchange(parts, [(box, got)], box_send, box_recv)
    for s in streams:
        s.drain()


def sum_and_exchange(npx, npy, box, part_one, part_two, collective_id):
    parts = npx * npy
    vmem = pl.BlockSpec(memory_space=pltpu.VMEM)
    _, height, width = part_one.shape
    orders = reduce_orders(npx, npy)
    scratch = []
    for order in orders:
        curs, recvs = scratch_for(order, parts, height, width)
        scratch += curs + recvs
    count = 2 * 2 * sum(size - 1 for _, _, size in orders[0])
    dma = pltpu.SemaphoreType.DMA
    return pl.pallas_call(
        functools.partial(sum_kernel, npx, npy),
        out_shape=tuple(
            jax.ShapeDtypeStruct(a.shape, a.dtype) for a in (box, part_one, part_two)
        ),
        in_specs=[vmem] * 3,
        out_specs=(vmem,) * 3,
        scratch_shapes=scratch + [dma((1,)), dma((1,)), dma((count,)), dma((count,))],
        compiler_params=pltpu.CompilerParams(
            collective_id=collective_id, has_side_effects=True, vmem_limit_bytes=56 * 2**20
        ),
        name="sum_and_exchange",
    )(box, part_one, part_two)


def dense_kernel(rows, cols, live, tiles, own, rest, total):
    row_tiles, col_tiles, tile, _ = total.shape
    total[...] = jnp.zeros_like(total)

    def add(t, carry):
        r, c = rows[0, t], cols[0, t]
        total[r, c] += tiles[t].astype(F32)
        return carry

    lax.fori_loop(0, live[0], add, 0)
    for r in range(row_tiles):
        for c in range(col_tiles):
            out, at = (own, c) if c < row_tiles else (rest, c - row_tiles)
            out[r * tile : (r + 1) * tile, at * tile : (at + 1) * tile] = total[r, c].astype(BF16)


def dense_tiles(tile_values, tile_rows, tile_cols, tile_count, row_tiles, col_tiles):
    tile = tile_values.shape[1]
    vmem = pl.BlockSpec(memory_space=pltpu.VMEM)
    smem = pl.BlockSpec(memory_space=pltpu.SMEM)
    rows = row_tiles * tile
    return pl.pallas_call(
        dense_kernel,
        out_shape=(
            jax.ShapeDtypeStruct((rows, rows), BF16),
            jax.ShapeDtypeStruct((rows, (col_tiles - row_tiles) * tile), BF16),
        ),
        in_specs=[smem, smem, smem, vmem],
        out_specs=(vmem, vmem),
        scratch_shapes=[pltpu.VMEM((row_tiles, col_tiles, tile, tile), F32)],
        compiler_params=pltpu.CompilerParams(vmem_limit_bytes=32 * 2**20),
        name="dense_tiles",
    )(tile_rows, tile_cols, tile_count, tile_values)


def dot(a, b, ca=1, cb=0):
    return lax.dot_general(a, b, (((ca,), (cb,)), ((), ())), preferred_element_type=F32)


def local(
    npx,
    npy,
    features,
    weight_one,
    weight_two,
    tile_values,
    tile_rows,
    tile_cols,
    tile_count,
    send_rows,
    send_count,
    stale_hidden,
    stale_grad,
    out_grad,
):
    parts = npx * npy
    rows_own, width = features.shape
    slots = send_rows.shape[2]
    tile = tile_values.shape[1]
    row_tiles = rows_own // tile
    col_tiles = (rows_own + parts * slots) // tile
    counts = send_count[0]
    slot_ids = jnp.arange(slots, dtype=jnp.int32)
    sent = (slot_ids[None, :] < counts[:, None]).reshape(-1)
    chosen = jnp.where(sent, send_rows[0].reshape(-1), -1)
    pick = (chosen[:, None] == jnp.arange(rows_own, dtype=jnp.int32)[None, :]).astype(BF16)
    own, rest = dense_tiles(tile_values, tile_rows, tile_cols, tile_count, row_tiles, col_tiles)

    down = dot(out_grad, weight_two, 1, 1).astype(BF16)
    box_g = dot(rest, down, 0, 0).astype(BF16)
    box_x = dot(pick, features).astype(BF16)
    box_n = jnp.broadcast_to(counts[:, None, None], (parts, 1, 128))
    in_x, in_g, in_n = exchange(
        npx,
        npy,
        (box_x.reshape(parts, slots, width), box_g.reshape(parts, slots, width), box_n),
        0,
    )
    heard = slot_ids[None, :] < in_n[:, 0, :1]
    agg_one = (dot(own, features) + dot(rest, in_x.reshape(-1, width))).astype(BF16)
    pre_one = dot(agg_one, weight_one)
    cdf = 0.5 * (1.0 + lax.erf(pre_one * (1.0 / math.sqrt(2.0))))
    hidden = (pre_one * cdf).astype(BF16)
    slope = cdf + pre_one * (jnp.exp(-0.5 * pre_one * pre_one) * (1.0 / math.sqrt(2.0 * math.pi)))
    box_h = dot(pick, hidden).astype(BF16)
    kept = jnp.where(heard.reshape(-1, 1), stale_hidden, jnp.zeros_like(stale_hidden))
    agg_two = (dot(own, hidden) + dot(rest, kept)).astype(BF16)
    hidden_grad = dot(own, down, 0, 0) + dot(pick, stale_grad, 0, 0)
    pre_grad = (hidden_grad * slope).astype(BF16)
    part_one = dot(agg_one, pre_grad, 0, 0).astype(BF16)
    part_two = dot(agg_two, out_grad, 0, 0).astype(BF16)

    height = -(-width // (8 * parts)) * 8
    pad = height * parts - width

    def cut(a):
        return jnp.pad(a, ((0, pad), (0, 0))).reshape(parts, height, width)

    got, sum_one, sum_two = sum_and_exchange(
        npx, npy, box_h.reshape(parts, slots, width), cut(part_one), cut(part_two), 1
    )
    scale = 1.0 / math.sqrt(rows_own * parts)

    def whole(a):
        return a.reshape(-1, width)[:width].astype(F32) * scale

    in_g = in_g.reshape(-1, width)
    next_grad = jnp.where(sent[:, None], in_g, jnp.zeros_like(in_g))
    return got.reshape(-1, width), next_grad, whole(sum_one), whole(sum_two)


def solution(mesh):
    in_specs = (
        P(("px", "py"), None),
        P(),
        P(),
        P(("px", "py"), None, None),
        P(("px", "py"), None),
        P(("px", "py"), None),
        P(("px", "py")),
        P(("px", "py"), None, None),
        P(("px", "py"), None),
        P(("px", "py"), None),
        P(("px", "py"), None),
        P(("px", "py"), None),
    )
    out_specs = (P(("px", "py"), None), P(("px", "py"), None), P(), P())
    body = functools.partial(local, mesh.shape["px"], mesh.shape["py"])
    return jax.shard_map(body, mesh=mesh, in_specs=in_specs, out_specs=out_specs, check_vma=False)
```

```python
import functools
import math

import jax
import jax.numpy as jnp
from jax import lax
from jax.experimental import pallas as pl
from jax.experimental.pallas import tpu as pltpu
from jax.sharding import PartitionSpec as P

MESH = pl.DeviceIdType.MESH
BF16 = jnp.bfloat16
F32 = jnp.float32


def split_axis(size):
    out, stride = [], 1
    while size > 1:
        two = size & (size - 1) == 0
        step = size if not two else (2 if (size.bit_length() - 1) % 2 else 4)
        out.append((stride, step))
        stride *= step
        size //= step
    return out


def positions(npx, npy):
    px, py = lax.axis_index("px"), lax.axis_index("py")
    return px, py, px * npy + py


def entry_barrier(me, npx, npy):
    parts = npx * npy
    barrier = pltpu.get_barrier_semaphore()

    def greet(step, carry):
        peer = lax.rem(me + step, parts)
        pl.semaphore_signal(
            barrier, inc=1, device_id=(peer // npy, lax.rem(peer, npy)), device_id_type=MESH
        )
        return carry

    lax.fori_loop(1, parts, greet, 0)
    pl.semaphore_wait(barrier, parts - 1)


def start_exchange(me, npx, npy, pairs, send_sem, recv_sem):
    parts = npx * npy

    def send(step, carry):
        peer = lax.rem(me + step, parts)
        for k, (src, dst) in enumerate(pairs):
            pltpu.make_async_remote_copy(
                src_ref=src.at[peer],
                dst_ref=dst.at[me],
                send_sem=send_sem.at[k],
                recv_sem=recv_sem.at[k],
                device_id=(peer // npy, lax.rem(peer, npy)),
                device_id_type=MESH,
            ).start()
        return carry

    lax.fori_loop(1, parts, send, 0)
    for src, dst in pairs:
        dst[me] = src[me]


def finish_exchange(parts, pairs, send_sem, recv_sem):
    for k, (src, dst) in enumerate(pairs):
        part_of = dst.at[pl.ds(0, parts - 1)]
        pltpu.make_async_copy(part_of, part_of, recv_sem.at[k]).wait()
        part_of = src.at[pl.ds(0, parts - 1)]
        pltpu.make_async_copy(part_of, part_of, send_sem.at[k]).wait()


def reduce_orders(npx, npy):
    dims = [("py", s, k) for s, k in split_axis(npy)] + [("px", s, k) for s, k in split_axis(npx)]
    near = [d for d in dims if d[2] == 2]
    far = [d for d in dims if d[2] != 2]
    return [near + far, near + far[::-1]]


class Stream:
    def __init__(self, order, parts, px, py, src, out, curs, recvs, sems):
        self.order, self.src, self.out, self.curs, self.recvs = order, src, out, curs, recvs
        self.send_sem, self.recv_sem, self.at = sems
        self.px, self.py = px, py
        self.coord, self.span, left = [], [], parts
        for axis, stride, size in order:
            index = px if axis == "px" else py
            self.coord.append(lax.rem(index // stride, size))
            left //= size
            self.span.append(left)
        self.base, total = [], 0
        for c, n in zip(self.coord, self.span):
            total = total + c * n
            self.base.append(total)
        self.live = {}

    def peer(self, stage, offset):
        axis, stride, size = self.order[stage]
        mine = self.coord[stage]
        other = lax.rem(mine + offset, size)
        move = (other - mine) * stride
        where = (self.px + move, self.py) if axis == "px" else (self.px, self.py + move)
        return other, where

    def copies(self, key, stage, make):
        made = []
        for offset in range(1, self.order[stage][2]):
            other, where = self.peer(stage, offset)
            src, dst = make(offset, other)
            copy = pltpu.make_async_remote_copy(
                src_ref=src,
                dst_ref=dst,
                send_sem=self.send_sem.at[self.at],
                recv_sem=self.recv_sem.at[self.at],
                device_id=where,
                device_id_type=MESH,
            )
            self.at += 1
            copy.start()
            made.append(copy)
        self.live[key] = made

    def scatter_start(self, stage):
        n = self.span[stage]
        cur = self.src if stage == 0 else self.curs[stage - 1]
        self.copies(
            ("rs", stage),
            stage,
            lambda offset, other: (cur.at[pl.ds(other * n, n)], self.recvs[stage].at[offset - 1]),
        )

    def scatter_finish(self, stage):
        n = self.span[stage]
        cur = self.src if stage == 0 else self.curs[stage - 1]
        last = stage == len(self.order) - 1
        target = self.out if last else self.curs[stage]
        start = self.base[stage] if last else 0
        for copy in self.live[("rs", stage)]:
            copy.wait_recv()
        mine = self.coord[stage] * n
        size = self.order[stage][2]

        def add(i, carry):
            total = cur[mine + i].astype(F32)
            for offset in range(1, size):
                total = total + self.recvs[stage][offset - 1, i].astype(F32)
            target[start + i] = total.astype(BF16)
            return carry

        lax.fori_loop(0, n, add, 0)

    def gather_start(self, stage):
        n = self.span[stage]
        block = self.out.at[pl.ds(self.base[stage], n)]
        self.copies(("ag", stage), stage, lambda offset, other: (block, block))

    def gather_finish(self, stage):
        for copy in self.live[("ag", stage)]:
            copy.wait_recv()

    def drain(self):
        for made in self.live.values():
            for copy in made:
                copy.wait_send()


def scratch_for(order, parts, height, width):
    curs, recvs, left = [], [], parts
    for stage, (_, _, size) in enumerate(order):
        left //= size
        recvs.append(pltpu.VMEM((size - 1, left, height, width), BF16))
        if stage < len(order) - 1:
            curs.append(pltpu.VMEM((left, height, width), BF16))
    return curs, recvs


def dot(a, b, ca=1, cb=0):
    return lax.dot_general(a, b, (((ca,), (cb,)), ((), ())), preferred_element_type=F32)


def dense_kernel(rows, cols, live, tiles, chosen, features, own, rest, pick, box, total):
    row_tiles, col_tiles, tile, _ = total.shape
    slots = box.shape[1]
    node = lax.broadcasted_iota(jnp.int32, pick.shape, 0)
    pick[...] = (node == chosen[...]).astype(F32).astype(BF16)
    out = dot(pick[...], features[...], 0, 0)
    box[...] = out.reshape(-1, slots, out.shape[1]).astype(BF16)
    total[...] = jnp.zeros_like(total)

    def add(t, carry):
        r, c = rows[0, t], cols[0, t]
        total[r, c] += tiles[t].astype(F32)
        return carry

    lax.fori_loop(0, live[0], add, 0)
    for r in range(row_tiles):
        for c in range(col_tiles):
            out, at = (own, c) if c < row_tiles else (rest, c - row_tiles)
            out[r * tile : (r + 1) * tile, at * tile : (at + 1) * tile] = total[r, c].astype(BF16)


def dense_tiles(tile_values, tile_rows, tile_cols, tile_count, chosen, features, parts):
    tile = tile_values.shape[1]
    rows, width = features.shape
    boundary = chosen.shape[1]
    vmem = pl.BlockSpec(memory_space=pltpu.VMEM)
    smem = pl.BlockSpec(memory_space=pltpu.SMEM)
    return pl.pallas_call(
        dense_kernel,
        out_shape=(
            jax.ShapeDtypeStruct((rows, rows), BF16),
            jax.ShapeDtypeStruct((rows, boundary), BF16),
            jax.ShapeDtypeStruct((rows, boundary), BF16),
            jax.ShapeDtypeStruct((parts, boundary // parts, width), BF16),
        ),
        in_specs=[smem, smem, smem, vmem, vmem, vmem],
        out_specs=(vmem,) * 4,
        scratch_shapes=[pltpu.VMEM((rows // tile, (rows + boundary) // tile, tile, tile), F32)],
        compiler_params=pltpu.CompilerParams(vmem_limit_bytes=32 * 2**20),
        name="dense_tiles",
    )(tile_rows, tile_cols, tile_count, tile_values, chosen, features)


def cuts(width, parts):
    first = width // 3 * 2
    out = []
    for start, size in ((0, first), (first, width - first)):
        out.append((start, size, -(-size // (8 * parts)) * 8))
    return out


def step_kernel(npx, npy, *refs):
    (counts, own, rest, pick, box_x) = refs[:5]
    hbm = refs[5:11]
    got_h, got_g = refs[11:13]
    parts = npx * npy
    width = own.shape[0]
    pieces = cuts(width, parts)
    outs = refs[13:17]
    (
        features,
        w_two,
        out_grad,
        stale_g,
        w_one,
        stale_h,
        down,
        agg_own,
        hidden_grad,
        box_g,
        box_h,
        box_n,
        in_x,
        in_n,
        agg_one,
        hidden,
        pre_grad,
        agg_two,
    ) = refs[17:35]
    srcs = refs[35:39]
    scratch = refs[39:-5]
    load_sem, ex_send, ex_recv, red_send, red_recv = refs[-5:]
    slots = box_x.shape[1]
    px, py, me = positions(npx, npy)

    held = (features, w_two, out_grad, stale_g, w_one, stale_h)
    loads = [pltpu.make_async_copy(a, b, load_sem.at[i]) for i, (a, b) in enumerate(zip(hbm, held))]
    for copy in loads:
        copy.start()

    def fill(q, carry):
        box_n[q] = jnp.full(box_n.shape[1:], counts[0, q], jnp.int32)
        return carry

    lax.fori_loop(0, parts, fill, 0)
    entry_barrier(me, npx, npy)
    sem = lambda i, n: (ex_send.at[pl.ds(i, n)], ex_recv.at[pl.ds(i, n)])
    pairs_x = [(box_x, in_x), (box_n, in_n)]
    start_exchange(me, npx, npy, pairs_x, *sem(0, 2))

    block = width // 3

    def rows_of(i):
        return pl.ds(pl.multiple_of(i * block, 128), block)

    for copy in loads[:4]:
        copy.wait()

    def early(i, carry):
        r = rows_of(i)
        down[r, :] = dot(out_grad[r, :], w_two[...], 1, 1).astype(BF16)
        agg_own[r, :] = dot(own[r, :], features[...])
        return carry

    lax.fori_loop(0, 3, early, 0)
    back = dot(rest[...], down[...], 0, 0)
    box_g[...] = back.reshape(parts, slots, width).astype(BF16)

    def back_step(i, carry):
        r = rows_of(i)
        hidden_grad[r, :] = dot(own[:, r], down[...], 0, 0) + dot(pick[r, :], stale_g[...])
        return carry

    lax.fori_loop(0, 3, back_step, 0)
    for copy in loads[4:]:
        copy.wait()
    finish_exchange(parts, pairs_x, *sem(0, 2))
    pairs_g = [(box_g, got_g)]
    start_exchange(me, npx, npy, pairs_g, *sem(2, 1))

    arrived = in_x[...].astype(F32).reshape(parts * slots, width).astype(BF16)

    def layer_one(i, carry):
        r = rows_of(i)
        agg = (agg_own[r, :] + dot(rest[r, :], arrived)).astype(BF16)
        agg_one[r, :] = agg
        v = dot(agg, w_one[...])
        cdf = 0.5 * (1.0 + lax.erf(v * (1.0 / math.sqrt(2.0))))
        hidden[r, :] = (v * cdf).astype(BF16)
        slope = cdf + v * (jnp.exp(-0.5 * v * v) * (1.0 / math.sqrt(2.0 * math.pi)))
        pre_grad[r, :] = (hidden_grad[r, :] * slope).astype(BF16)
        return carry

    lax.fori_loop(0, 3, layer_one, 0)
    box = dot(pick[...], hidden[...], 0, 0)
    box_h[...] = box.reshape(parts, slots, width).astype(BF16)
    pairs_h = [(box_h, got_h)]
    start_exchange(me, npx, npy, pairs_h, *sem(3, 1))

    orders = reduce_orders(npx, npy)
    stages = len(orders[0])
    per = 2 * sum(size - 1 for _, _, size in orders[0]) // 2
    streams, at = [], 0
    for k in range(4):
        curs = scratch[at : at + stages - 1]
        recvs = scratch[at + stages - 1 : at + 2 * stages - 1]
        at += 2 * stages - 1
        sems = (red_send, red_recv, 2 * k * per)
        streams.append(Stream(orders[k % 2], parts, px, py, srcs[k], outs[k], curs, recvs, sems))

    def weight_grad(left, right, targets):
        for (start, size, height), target in zip(pieces, targets):
            for low in range(start, start + size, 128):
                part = dot(left[:, low : low + 128], right[...], 0, 0)
                c = (low - start) // height
                n = 128 // height
                target[c : c + n] = part.reshape(n, height, width).astype(BF16)
            full = size // height
            if full < parts:
                target[full:] = jnp.zeros((parts - full,) + target.shape[1:], BF16)

    weight_grad(agg_one, pre_grad, srcs[:2])
    for s in streams[:2]:
        s.scatter_start(0)

    slot = lax.broadcasted_iota(jnp.int32, (parts, slots, 128), 1)
    heard = slot < in_n[...]
    kept = []
    for low in range(0, width, 128):
        piece = stale_h[:, :, low : low + 128].astype(F32)
        kept.append(jnp.where(heard, piece, 0.0).reshape(parts * slots, 128).astype(BF16))
    kept = jnp.concatenate(kept, axis=1)

    def layer_two(i, carry):
        r = rows_of(i)
        agg_two[r, :] = (dot(own[r, :], hidden[...]) + dot(rest[r, :], kept)).astype(BF16)
        return carry

    lax.fori_loop(0, 3, layer_two, 0)
    for s in streams[:2]:
        s.scatter_finish(0)
        s.scatter_start(1)
    weight_grad(agg_two, out_grad, srcs[2:])
    for s in streams[2:]:
        s.scatter_start(0)
    for s in streams[2:]:
        s.scatter_finish(0)
        s.scatter_start(1)

    for stage in range(1, stages):
        for s in streams:
            s.scatter_finish(stage)
            if stage < stages - 1:
                s.scatter_start(stage + 1)
            else:
                s.gather_start(stage)
    for stage in range(stages - 1, -1, -1):
        for s in streams:
            s.gather_finish(stage)
            if stage > 0:
                s.gather_start(stage - 1)
    finish_exchange(parts, pairs_g, *sem(2, 1))
    finish_exchange(parts, pairs_h, *sem(3, 1))
    for s in streams:
        s.drain()


def step(npx, npy, counts, own, rest, pick, box_x, held):
    parts = npx * npy
    vmem = pl.BlockSpec(memory_space=pltpu.VMEM)
    smem = pl.BlockSpec(memory_space=pltpu.SMEM)
    hbm = pl.BlockSpec(memory_space=pl.ANY)
    width = own.shape[0]
    pieces = cuts(width, parts)
    orders = reduce_orders(npx, npy)
    heights = [p[2] for p in pieces] * 2
    chunked = [(parts, h, width) for h in heights]
    scratch = []
    for k in range(4):
        curs, recvs = scratch_for(orders[k % 2], parts, heights[k], width)
        scratch += curs + recvs
    count = 4 * 2 * sum(size - 1 for _, _, size in orders[0])
    dma = pltpu.SemaphoreType.DMA
    square = (width, width)
    box = box_x.shape
    mine = [pltpu.VMEM(a.shape, a.dtype) for a in held]
    mine += [pltpu.VMEM(square, BF16), pltpu.VMEM(square, F32), pltpu.VMEM(square, F32)]
    mine += [pltpu.VMEM(box, BF16), pltpu.VMEM(box, BF16)]
    mine += [pltpu.VMEM((parts, 1, 128), jnp.int32), pltpu.VMEM(box, BF16)]
    mine += [pltpu.VMEM((parts, 1, 128), jnp.int32)]
    mine += [pltpu.VMEM(square, BF16)] * 4
    mine += [pltpu.VMEM(c, BF16) for c in chunked]
    return pl.pallas_call(
        functools.partial(step_kernel, npx, npy),
        out_shape=tuple(jax.ShapeDtypeStruct(c, BF16) for c in [box, box] + chunked),
        in_specs=[smem] + [vmem] * 4 + [hbm] * 6,
        out_specs=(vmem,) * 6,
        scratch_shapes=mine + scratch + [dma((6,)), dma((4,)), dma((4,)), dma((count,)), dma((count,))],
        compiler_params=pltpu.CompilerParams(
            collective_id=0,
            has_side_effects=True,
            vmem_limit_bytes=min(36 + 26 * parts // 128, 62) * 2**20,
        ),
        name="graph_step",
    )(counts, own, rest, pick, box_x, *held)


def local(
    npx,
    npy,
    features,
    weight_one,
    weight_two,
    tile_values,
    tile_rows,
    tile_cols,
    tile_count,
    send_rows,
    send_count,
    stale_hidden,
    stale_grad,
    out_grad,
):
    parts = npx * npy
    rows_own, width = features.shape
    slots = send_rows.shape[2]
    slot_ids = jnp.arange(slots, dtype=jnp.int32)
    sent = (slot_ids[None, :] < send_count[0][:, None]).reshape(-1)
    chosen = jnp.where(sent, send_rows[0].reshape(-1), -1).reshape(1, -1)
    own, rest, pick, box_x = dense_tiles(
        tile_values, tile_rows, tile_cols, tile_count, chosen, features, parts
    )
    held = (
        features,
        weight_two,
        out_grad,
        stale_grad,
        weight_one,
        stale_hidden.reshape(parts, slots, width),
    )
    got_h, got_g, *sums = step(npx, npy, send_count, own, rest, pick, box_x, held)
    scale = 1.0 / math.sqrt(rows_own * parts)
    pieces = cuts(width, parts)

    def whole(blocks):
        flat = [a.reshape(-1, width)[: p[1]] for a, p in zip(blocks, pieces)]
        return jnp.concatenate(flat, axis=0).astype(F32) * scale

    got_g = got_g.reshape(-1, width)
    next_grad = jnp.where(sent[:, None], got_g, jnp.zeros_like(got_g))
    return got_h.reshape(-1, width), next_grad, whole(sums[:2]), whole(sums[2:])


def solution(mesh):
    in_specs = (
        P(("px", "py"), None),
        P(),
        P(),
        P(("px", "py"), None, None),
        P(("px", "py"), None),
        P(("px", "py"), None),
        P(("px", "py")),
        P(("px", "py"), None, None),
        P(("px", "py"), None),
        P(("px", "py"), None),
        P(("px", "py"), None),
        P(("px", "py"), None),
    )
    out_specs = (P(("px", "py"), None), P(("px", "py"), None), P(), P())
    body = functools.partial(local, mesh.shape["px"], mesh.shape["py"])
    return jax.shard_map(body, mesh=mesh, in_specs=in_specs, out_specs=out_specs, check_vma=False)
```

```python
import functools
import math

import jax
import jax.numpy as jnp
from jax import lax
from jax.experimental import pallas as pl
from jax.experimental.pallas import tpu as pltpu
from jax.sharding import PartitionSpec as P

MESH = pl.DeviceIdType.MESH
BF16 = jnp.bfloat16
F32 = jnp.float32


def split_axis(size):
    out, stride = [], 1
    while size > 1:
        two = size & (size - 1) == 0
        step = size if not two else (2 if (size.bit_length() - 1) % 2 else 4)
        out.append((stride, step))
        stride *= step
        size //= step
    return out


def positions(npx, npy):
    px, py = lax.axis_index("px"), lax.axis_index("py")
    return px, py, px * npy + py


def entry_barrier(me, npx, npy):
    parts = npx * npy
    barrier = pltpu.get_barrier_semaphore()

    def greet(step, carry):
        peer = lax.rem(me + step, parts)
        pl.semaphore_signal(
            barrier, inc=1, device_id=(peer // npy, lax.rem(peer, npy)), device_id_type=MESH
        )
        return carry

    lax.fori_loop(1, parts, greet, 0)
    pl.semaphore_wait(barrier, parts - 1)


def start_exchange(me, npx, npy, pairs, send_sem, recv_sem):
    parts = npx * npy

    def send(step, carry):
        peer = lax.rem(me + step, parts)
        for k, (src, dst) in enumerate(pairs):
            pltpu.make_async_remote_copy(
                src_ref=src.at[peer],
                dst_ref=dst.at[me],
                send_sem=send_sem.at[k],
                recv_sem=recv_sem.at[k],
                device_id=(peer // npy, lax.rem(peer, npy)),
                device_id_type=MESH,
            ).start()
        return carry

    lax.fori_loop(1, parts, send, 0)
    for src, dst in pairs:
        dst[me] = src[me]


def finish_exchange(parts, pairs, send_sem, recv_sem):
    for k, (src, dst) in enumerate(pairs):
        part_of = dst.at[pl.ds(0, parts - 1)]
        pltpu.make_async_copy(part_of, part_of, recv_sem.at[k]).wait()
        part_of = src.at[pl.ds(0, parts - 1)]
        pltpu.make_async_copy(part_of, part_of, send_sem.at[k]).wait()


def reduce_orders(npx, npy):
    dims = [("py", s, k) for s, k in split_axis(npy)] + [("px", s, k) for s, k in split_axis(npx)]
    near = [d for d in dims if d[2] == 2]
    far = [d for d in dims if d[2] != 2]
    return [near + far, near + far[::-1]]


class Stream:
    def __init__(self, order, parts, px, py, src, out, curs, recvs, sems):
        self.order, self.src, self.out, self.curs, self.recvs = order, src, out, curs, recvs
        self.send_sem, self.recv_sem, self.at = sems
        self.px, self.py = px, py
        self.coord, self.span, left = [], [], parts
        for axis, stride, size in order:
            index = px if axis == "px" else py
            self.coord.append(lax.rem(index // stride, size))
            left //= size
            self.span.append(left)
        self.base, total = [], 0
        for c, n in zip(self.coord, self.span):
            total = total + c * n
            self.base.append(total)
        self.live = {}

    def peer(self, stage, offset):
        axis, stride, size = self.order[stage]
        mine = self.coord[stage]
        other = lax.rem(mine + offset, size)
        move = (other - mine) * stride
        where = (self.px + move, self.py) if axis == "px" else (self.px, self.py + move)
        return other, where

    def copies(self, key, stage, make):
        made = []
        for offset in range(1, self.order[stage][2]):
            other, where = self.peer(stage, offset)
            src, dst = make(offset, other)
            copy = pltpu.make_async_remote_copy(
                src_ref=src,
                dst_ref=dst,
                send_sem=self.send_sem.at[self.at],
                recv_sem=self.recv_sem.at[self.at],
                device_id=where,
                device_id_type=MESH,
            )
            self.at += 1
            copy.start()
            made.append(copy)
        self.live[key] = made

    def scatter_start(self, stage):
        n = self.span[stage]
        cur = self.src if stage == 0 else self.curs[stage - 1]
        self.copies(
            ("rs", stage),
            stage,
            lambda offset, other: (cur.at[pl.ds(other * n, n)], self.recvs[stage].at[offset - 1]),
        )

    def scatter_finish(self, stage):
        n = self.span[stage]
        cur = self.src if stage == 0 else self.curs[stage - 1]
        last = stage == len(self.order) - 1
        target = self.out if last else self.curs[stage]
        start = self.base[stage] if last else 0
        for copy in self.live[("rs", stage)]:
            copy.wait_recv()
        mine = self.coord[stage] * n
        size = self.order[stage][2]

        def add(i, carry):
            total = cur[mine + i].astype(F32)
            for offset in range(1, size):
                total = total + self.recvs[stage][offset - 1, i].astype(F32)
            target[start + i] = total.astype(BF16)
            return carry

        lax.fori_loop(0, n, add, 0)

    def gather_start(self, stage):
        n = self.span[stage]
        block = self.out.at[pl.ds(self.base[stage], n)]
        self.copies(("ag", stage), stage, lambda offset, other: (block, block))

    def gather_finish(self, stage):
        for copy in self.live[("ag", stage)]:
            copy.wait_recv()

    def drain(self):
        for made in self.live.values():
            for copy in made:
                copy.wait_send()


def scratch_for(order, parts, height, width):
    curs, recvs, left = [], [], parts
    for stage, (_, _, size) in enumerate(order):
        left //= size
        recvs.append(pltpu.VMEM((size - 1, left, height, width), BF16))
        if stage < len(order) - 1:
            curs.append(pltpu.VMEM((left, height, width), BF16))
    return curs, recvs


def dot(a, b, ca=1, cb=0):
    return lax.dot_general(a, b, (((ca,), (cb,)), ((), ())), preferred_element_type=F32)


def dense_kernel(rows, cols, live, tiles, chosen, features, own, rest, pick, box, total):
    row_tiles, col_tiles, tile, _ = total.shape
    slots = box.shape[1]
    node = lax.broadcasted_iota(jnp.int32, pick.shape, 0)
    pick[...] = (node == chosen[...]).astype(F32).astype(BF16)
    out = dot(pick[...], features[...], 0, 0)
    box[...] = out.reshape(-1, slots, out.shape[1]).astype(BF16)
    total[...] = jnp.zeros_like(total)

    def add(t, carry):
        r, c = rows[0, t], cols[0, t]
        total[r, c] += tiles[t].astype(F32)
        return carry

    lax.fori_loop(0, live[0], add, 0)
    for r in range(row_tiles):
        for c in range(col_tiles):
            out, at = (own, c) if c < row_tiles else (rest, c - row_tiles)
            out[r * tile : (r + 1) * tile, at * tile : (at + 1) * tile] = total[r, c].astype(BF16)


def dense_tiles(tile_values, tile_rows, tile_cols, tile_count, chosen, features, parts):
    tile = tile_values.shape[1]
    rows, width = features.shape
    boundary = chosen.shape[1]
    vmem = pl.BlockSpec(memory_space=pltpu.VMEM)
    smem = pl.BlockSpec(memory_space=pltpu.SMEM)
    return pl.pallas_call(
        dense_kernel,
        out_shape=(
            jax.ShapeDtypeStruct((rows, rows), BF16),
            jax.ShapeDtypeStruct((rows, boundary), BF16),
            jax.ShapeDtypeStruct((rows, boundary), BF16),
            jax.ShapeDtypeStruct((parts, boundary // parts, width), BF16),
        ),
        in_specs=[smem, smem, smem, vmem, vmem, vmem],
        out_specs=(vmem,) * 4,
        scratch_shapes=[pltpu.VMEM((rows // tile, (rows + boundary) // tile, tile, tile), F32)],
        compiler_params=pltpu.CompilerParams(vmem_limit_bytes=32 * 2**20),
        name="dense_tiles",
    )(tile_rows, tile_cols, tile_count, tile_values, chosen, features)


def cuts(width, parts):
    first = width // 3 * 2
    out = []
    for start, size in ((0, first), (first, width - first)):
        out.append((start, size, -(-size // (8 * parts)) * 8))
    return out


def step_kernel(npx, npy, *refs):
    (counts, own, rest, pick, box_x) = refs[:5]
    hbm = refs[5:11]
    got_h, got_g = refs[11:13]
    parts = npx * npy
    width = own.shape[0]
    pieces = cuts(width, parts)
    outs = refs[13:17]
    (
        features,
        w_two,
        out_grad,
        stale_g,
        w_one,
        stale_h,
        down,
        agg_own,
        hidden_grad,
        box_g,
        box_h,
        box_n,
        in_x,
        in_n,
        agg_one,
        hidden,
        pre_grad,
        agg_two,
    ) = refs[17:35]
    srcs = refs[35:39]
    scratch = refs[39:-5]
    load_sem, ex_send, ex_recv, red_send, red_recv = refs[-5:]
    slots = box_x.shape[1]
    px, py, me = positions(npx, npy)

    held = (features, w_two, out_grad, stale_g, w_one, stale_h)
    loads = [pltpu.make_async_copy(a, b, load_sem.at[i]) for i, (a, b) in enumerate(zip(hbm, held))]
    for copy in loads:
        copy.start()

    def fill(q, carry):
        box_n[q] = jnp.full(box_n.shape[1:], counts[0, q], jnp.int32)
        return carry

    lax.fori_loop(0, parts, fill, 0)
    entry_barrier(me, npx, npy)
    sem = lambda i, n: (ex_send.at[pl.ds(i, n)], ex_recv.at[pl.ds(i, n)])
    pairs_x = [(box_x, in_x), (box_n, in_n)]
    start_exchange(me, npx, npy, pairs_x, *sem(0, 2))

    block = width // 3

    def rows_of(i):
        return pl.ds(pl.multiple_of(i * block, 128), block)

    for copy in loads[:4]:
        copy.wait()

    def early(i, carry):
        r = rows_of(i)
        down[r, :] = dot(out_grad[r, :], w_two[...], 1, 1).astype(BF16)
        agg_own[r, :] = dot(own[r, :], features[...])
        return carry

    lax.fori_loop(0, 3, early, 0)
    back = dot(rest[...], down[...], 0, 0)
    box_g[...] = back.reshape(parts, slots, width).astype(BF16)

    def back_step(i, carry):
        r = rows_of(i)
        hidden_grad[r, :] = dot(own[:, r], down[...], 0, 0) + dot(pick[r, :], stale_g[...])
        return carry

    lax.fori_loop(0, 3, back_step, 0)
    for copy in loads[4:]:
        copy.wait()
    finish_exchange(parts, pairs_x, *sem(0, 2))
    pairs_g = [(box_g, got_g)]
    start_exchange(me, npx, npy, pairs_g, *sem(2, 1))

    arrived = in_x[...].astype(F32).reshape(parts * slots, width).astype(BF16)

    def layer_one(i, carry):
        r = rows_of(i)
        agg = (agg_own[r, :] + dot(rest[r, :], arrived)).astype(BF16)
        agg_one[r, :] = agg
        v = dot(agg, w_one[...])
        cdf = 0.5 * (1.0 + lax.erf(v * (1.0 / math.sqrt(2.0))))
        hidden[r, :] = (v * cdf).astype(BF16)
        slope = cdf + v * (jnp.exp(-0.5 * v * v) * (1.0 / math.sqrt(2.0 * math.pi)))
        pre_grad[r, :] = (hidden_grad[r, :] * slope).astype(BF16)
        return carry

    lax.fori_loop(0, 3, layer_one, 0)
    box = dot(pick[...], hidden[...], 0, 0)
    box_h[...] = box.reshape(parts, slots, width).astype(BF16)
    pairs_h = [(box_h, got_h)]
    start_exchange(me, npx, npy, pairs_h, *sem(3, 1))

    orders = reduce_orders(npx, npy)
    stages = len(orders[0])
    per = 2 * sum(size - 1 for _, _, size in orders[0]) // 2
    streams, at = [], 0
    for k in range(4):
        curs = scratch[at : at + stages - 1]
        recvs = scratch[at + stages - 1 : at + 2 * stages - 1]
        at += 2 * stages - 1
        sems = (red_send, red_recv, 2 * k * per)
        streams.append(Stream(orders[k % 2], parts, px, py, srcs[k], outs[k], curs, recvs, sems))

    def weight_grad(left, right, targets):
        for (start, size, height), target in zip(pieces, targets):
            for low in range(start, start + size, 128):
                part = dot(left[:, low : low + 128], right[...], 0, 0)
                c = (low - start) // height
                n = 128 // height
                target[c : c + n] = part.reshape(n, height, width).astype(BF16)
            full = size // height
            if full < parts:
                target[full:] = jnp.zeros((parts - full,) + target.shape[1:], BF16)

    weight_grad(agg_one, pre_grad, srcs[:2])
    for s in streams[:2]:
        s.scatter_start(0)

    slot = lax.broadcasted_iota(jnp.int32, (parts, slots, 128), 1)
    heard = slot < in_n[...]
    kept = []
    for low in range(0, width, 128):
        piece = stale_h[:, :, low : low + 128].astype(F32)
        kept.append(jnp.where(heard, piece, 0.0).reshape(parts * slots, 128).astype(BF16))
    kept = jnp.concatenate(kept, axis=1)

    def layer_two(i, carry):
        r = rows_of(i)
        agg_two[r, :] = (dot(own[r, :], hidden[...]) + dot(rest[r, :], kept)).astype(BF16)
        return carry

    lax.fori_loop(0, 3, layer_two, 0)
    for s in streams[:2]:
        s.scatter_finish(0)
        s.scatter_start(1)
    weight_grad(agg_two, out_grad, srcs[2:])
    for s in streams[2:]:
        s.scatter_start(0)
    for s in streams[2:]:
        s.scatter_finish(0)
        s.scatter_start(1)

    for stage in range(1, stages):
        for s in streams:
            s.scatter_finish(stage)
            if stage < stages - 1:
                s.scatter_start(stage + 1)
            else:
                s.gather_start(stage)
    for stage in range(stages - 1, -1, -1):
        for s in streams:
            s.gather_finish(stage)
            if stage > 0:
                s.gather_start(stage - 1)
    finish_exchange(parts, pairs_g, *sem(2, 1))
    finish_exchange(parts, pairs_h, *sem(3, 1))
    for s in streams:
        s.drain()


def step(npx, npy, counts, own, rest, pick, box_x, held):
    parts = npx * npy
    vmem = pl.BlockSpec(memory_space=pltpu.VMEM)
    smem = pl.BlockSpec(memory_space=pltpu.SMEM)
    hbm = pl.BlockSpec(memory_space=pltpu.HBM)
    width = own.shape[0]
    pieces = cuts(width, parts)
    orders = reduce_orders(npx, npy)
    heights = [p[2] for p in pieces] * 2
    chunked = [(parts, h, width) for h in heights]
    scratch = []
    for k in range(4):
        curs, recvs = scratch_for(orders[k % 2], parts, heights[k], width)
        scratch += curs + recvs
    count = 4 * 2 * sum(size - 1 for _, _, size in orders[0])
    dma = pltpu.SemaphoreType.DMA
    square = (width, width)
    box = box_x.shape
    mine = [pltpu.VMEM(a.shape, a.dtype) for a in held]
    mine += [pltpu.VMEM(square, BF16), pltpu.VMEM(square, F32), pltpu.VMEM(square, F32)]
    mine += [pltpu.VMEM(box, BF16), pltpu.VMEM(box, BF16)]
    mine += [pltpu.VMEM((parts, 1, 128), jnp.int32), pltpu.VMEM(box, BF16)]
    mine += [pltpu.VMEM((parts, 1, 128), jnp.int32)]
    mine += [pltpu.VMEM(square, BF16)] * 4
    mine += [pltpu.VMEM(c, BF16) for c in chunked]
    return pl.pallas_call(
        functools.partial(step_kernel, npx, npy),
        out_shape=tuple(jax.ShapeDtypeStruct(c, BF16) for c in [box, box] + chunked),
        in_specs=[smem] + [vmem] * 4 + [hbm] * 6,
        out_specs=(vmem,) * 6,
        scratch_shapes=mine + scratch + [dma((6,)), dma((4,)), dma((4,)), dma((count,)), dma((count,))],
        compiler_params=pltpu.CompilerParams(
            collective_id=0,
            has_side_effects=True,
            vmem_limit_bytes=min(50 + 8 * parts // 128, 62) * 2**20,
        ),
        name="graph_step",
    )(counts, own, rest, pick, box_x, *held)


def local(
    npx,
    npy,
    features,
    weight_one,
    weight_two,
    tile_values,
    tile_rows,
    tile_cols,
    tile_count,
    send_rows,
    send_count,
    stale_hidden,
    stale_grad,
    out_grad,
):
    parts = npx * npy
    rows_own, width = features.shape
    slots = send_rows.shape[2]
    slot_ids = jnp.arange(slots, dtype=jnp.int32)
    sent = (slot_ids[None, :] < send_count[0][:, None]).reshape(-1)
    chosen = jnp.where(sent, send_rows[0].reshape(-1), -1).reshape(1, -1)
    own, rest, pick, box_x = dense_tiles(
        tile_values, tile_rows, tile_cols, tile_count, chosen, features, parts
    )
    held = (
        features,
        weight_two,
        out_grad,
        stale_grad,
        weight_one,
        stale_hidden.reshape(parts, slots, width),
    )
    got_h, got_g, *sums = step(npx, npy, send_count, own, rest, pick, box_x, held)
    scale = 1.0 / math.sqrt(rows_own * parts)
    pieces = cuts(width, parts)

    def whole(blocks):
        flat = [a.reshape(-1, width)[: p[1]] for a, p in zip(blocks, pieces)]
        return jnp.concatenate(flat, axis=0).astype(F32) * scale

    got_g = got_g.reshape(-1, width)
    next_grad = jnp.where(sent[:, None], got_g, jnp.zeros_like(got_g))
    return got_h.reshape(-1, width), next_grad, whole(sums[:2]), whole(sums[2:])


def solution(mesh):
    in_specs = (
        P(("px", "py"), None),
        P(),
        P(),
        P(("px", "py"), None, None),
        P(("px", "py"), None),
        P(("px", "py"), None),
        P(("px", "py")),
        P(("px", "py"), None, None),
        P(("px", "py"), None),
        P(("px", "py"), None),
        P(("px", "py"), None),
        P(("px", "py"), None),
    )
    out_specs = (P(("px", "py"), None), P(("px", "py"), None), P(), P())
    body = functools.partial(local, mesh.shape["px"], mesh.shape["py"])
    return jax.shard_map(body, mesh=mesh, in_specs=in_specs, out_specs=out_specs, check_vma=False)
```
